512 devices in a mesh: grp: 8 (over y_lo, x), shard: 64 (over z, y_hi, core).
Axes of the slice: x: 4, y: 4 (y_hi: 2, y_lo: 2; y = y_hi * 2 + y_lo), z: 16, core: 2. Of those that a mesh axis runs over, the one named last changes fastest.
Arguments:
- window: bfloat16 [128, 4096], P('grp'), may hold values from -6 to 6
- weight: bfloat16 [11008, 4096], P('shard'), may hold values from -0.09375 to 0.09375
- factor_a: bfloat16 [1024, 4, 4096], P(('grp', 'shard')), may hold values from -6 to 6
- factor_b: bfloat16 [1024, 4, 11008], P(('grp', 'shard')), may hold values from -6 to 6
- fitness: float32 [1024], P(('grp', 'shard')), may hold values from -4 to 4
Outputs:
- perturbed: bfloat16 [11008, 16384], P('shard', 'grp')
- update: float32 [11008, 4096], P('shard', 'grp')
The draws below stay inside these ranges and needn't reach their ends.
All inputs are finite; a program needn't handle non-finite values.
Results may differ from the reference program's by a relative error of at most 0.0029.
Values may be sent and summed in bfloat16 or wider, within the bound.
No kernel may reach another device: no remote copies, remote signals or barrier semaphores. Data moves between devices by JAX's collectives and lax.ppermute only.
A program may use at most 64 MiB of HBM per device.

```python
import math
import jax
import jax.numpy as jnp
from jax import lax

D = 4096
FF = 11008
TOK = 16
RANK = 4
CANDS = 1024
N_GRP = 8


def levels(rng, extent, split, smallest, high):
    def one(dim, blocks):
        draws = jax.random.uniform(jax.random.fold_in(jax.random.fold_in(rng, 6), dim), (blocks,), jnp.float32, smallest / len(split), high / len(split))
        return jnp.repeat(jnp.exp(draws), extent[dim] // blocks).reshape((-1,) + (1,) * (len(extent) - dim - 1))

    level = one(*split[0])
    for cut in split[1:]:
        level = level * one(*cut)
    return level


def normal_values(own_key, shape, width, most, pieces=(), kind=jnp.bfloat16):
    gain = levels(own_key, shape, pieces, -0.22, 0.18) if pieces else 1.0
    values = jax.random.normal(own_key, shape, jnp.float32) * width * gain
    return jnp.minimum(jnp.maximum(values, -most), most).astype(kind)


def setup_inputs(seed: int = 0) -> dict:
    streams_of = jax.random.split(jax.random.key(seed), 6)
    window = normal_values(streams_of[0], (N_GRP * TOK, D), 1.0, 6.0, ((0, 8),))
    weight = normal_values(streams_of[1], (FF, D), D ** -0.5, 0.09375, ((0, 64),))
    factor_a = normal_values(streams_of[2], (CANDS, RANK, D), 1.0, 6.0, ((0, 512),))
    factor_b = normal_values(streams_of[3], (CANDS, RANK, FF), 1.0, 6.0, ((0, 512),))
    fitness = normal_values(streams_of[4], (CANDS,), 1.0, 4.0, ((0, 512),), jnp.float32)
    return {"window": window, "weight": weight, "factor_a": factor_a, "factor_b": factor_b, "fitness": fitness}


def reference(window, weight, factor_a, factor_b, fitness):
    total_cands = factor_a.shape[0]
    group_count = window.shape[0] // TOK
    per_group = total_cands // group_count
    perturb = 0.25 / math.sqrt(D)
    base_out = jnp.dot(window, weight.T, preferred_element_type=jnp.float32).reshape(group_count, TOK, FF)
    x_groups = window.reshape(group_count, TOK, D)
    a_groups = factor_a.reshape(group_count, per_group, RANK, D)
    b_groups = factor_b.reshape(group_count, per_group, RANK, FF)

    def one_group(inputs):
        group_window, group_a, group_b, group_base = inputs
        projected = jnp.einsum('td,crd->crt', group_window.astype(jnp.float32), group_a.astype(jnp.float32), precision=lax.Precision.HIGHEST)
        low_rank = jnp.einsum('crt,crf->ctf', projected, group_b.astype(jnp.float32), precision=lax.Precision.HIGHEST)
        return (group_base[None] + perturb * low_rank).astype(jnp.bfloat16)
    perturbed = lax.map(one_group, (x_groups, a_groups, b_groups, base_out)).reshape(total_cands * TOK, FF).T
    weighted = (fitness[:, None, None] * factor_b.astype(jnp.float32)).astype(jnp.bfloat16)
    update = jnp.dot(weighted.reshape(total_cands * RANK, FF).T, factor_a.reshape(total_cands * RANK, D), preferred_element_type=jnp.float32)
    update = update * (0.5 / math.sqrt(total_cands))
    return (perturbed, update)
```

```python
import functools
import math

import jax
import jax.numpy as jnp
from jax import lax
from jax.experimental import pallas as pl
from jax.experimental.pallas import tpu as pltpu
from jax.sharding import Mesh
from jax.sharding import PartitionSpec as P


F32, BF16 = jnp.float32, jnp.bfloat16
Q = ("yhi", "core")
SHARD = ("z", "yhi", "core")
GRP_SHARD = ("grp", "z", "yhi", "core")
LANE = 128
PARTS = 3
NT = (((1,), (1,)), ((), ()))


def up8(n):
    return (n + 7) // 8 * 8


def upl(n):
    return (n + LANE - 1) // LANE * LANE


def call(body, name, out_shape, args, flops, scratch=(), smem=()):
    vmem = pl.BlockSpec(memory_space=pltpu.VMEM)
    scalar = pl.BlockSpec(memory_space=pltpu.SMEM)
    many = isinstance(out_shape, (list, tuple))
    return pl.pallas_call(
        body,
        name=name,
        out_shape=out_shape,
        in_specs=[scalar if i in smem else vmem for i in range(len(args))],
        out_specs=[vmem] * len(out_shape) if many else vmem,
        scratch_shapes=list(scratch),
        cost_estimate=pl.CostEstimate(flops=flops, bytes_accessed=1 << 20, transcendentals=0),
        compiler_params=pltpu.CompilerParams(vmem_limit_bytes=40 << 20),
    )(*args)


def split3(x):
    hi = x.astype(BF16).astype(F32)
    rest = x - hi
    mid = rest.astype(BF16).astype(F32)
    return hi, mid, (rest - mid).astype(BF16).astype(F32)


def cut_a(a_ref, out_ref):
    groups, rows, width = out_ref.shape
    cands = a_ref.shape[0]
    rank = rows // cands
    for g in range(groups):
        columns = slice(g * width, (g + 1) * width)
        both = [a_ref[c, :, columns].astype(F32) for c in range(cands)]
        out_ref[g] = jnp.concatenate(both, axis=0).astype(BF16)


def pack_b(fit_ref, win_ref, a_ref, b_ref, out_ref, wide_ref):
    nz, rows, lanes = out_ref.shape
    cands, rank, hidden = b_ref.shape
    tok, depth = win_ref.shape
    nq = 4
    own = hidden // (nz * nq)
    step = up8(own)
    for c in range(cands):
        wide_ref[c * rank : (c + 1) * rank, :hidden] = b_ref[c].astype(F32)
    wide_ref[:, hidden:] = jnp.zeros((rows, wide_ref.shape[1] - hidden), F32)
    a_rows = jnp.concatenate([a_ref[c].astype(F32) for c in range(cands)], axis=0).astype(BF16)
    first = nq * step % LANE
    win = win_ref[...]
    spread = jnp.concatenate(
        [jnp.zeros((first, depth), BF16)]
        + [win] * PARTS
        + [jnp.zeros((LANE - first - PARTS * tok, depth), BF16)],
        axis=0,
    )
    proj = lax.dot_general(a_rows, spread, NT, preferred_element_type=F32)
    lane = lax.broadcasted_iota(jnp.int32, (rows, LANE), 1)
    row = lax.broadcasted_iota(jnp.int32, (rows, LANE), 0)
    hi, mid, lo = split3(proj)
    extra = jnp.where(lane < first + tok, hi, jnp.where(lane < first + 2 * tok, mid, lo))
    fit = jnp.where(row < rank, fit_ref[0], fit_ref[1])
    fhi, fmid, flo = split3(fit)
    at = first + PARTS * tok
    fits = jnp.where(lane == at, fhi, jnp.where(lane == at + 1, fmid, flo))
    extra = jnp.where(lane < at, extra, jnp.where(lane < at + 3, fits, 0.0))
    for z in range(nz):
        block = [jnp.zeros((rows, LANE), F32) for _ in range(lanes // LANE)]
        for q in range(nq):
            source = (z * nq + q) * own
            base = source // LANE * LANE
            target = q * step
            start = target // LANE
            offset = target % LANE
            span = min(3, len(block) - start)
            window = wide_ref[:, base : base + 3 * LANE]
            turn = (offset - (source - base)) % (3 * LANE)
            if turn:
                window = pltpu.roll(window, turn, 1)
            for k in range(span):
                at_lane = lane + k * LANE
                inside = (at_lane >= offset) & (at_lane < offset + own)
                piece = window[:, k * LANE : (k + 1) * LANE]
                block[start + k] = jnp.where(inside, piece, block[start + k])
        block[-1] = jnp.where(lane >= first, extra, block[-1])
        out_ref[z] = jnp.concatenate(block, axis=1).astype(BF16)


def turn_b(in_ref, w_ref, p_ref):
    nz, rows, lanes = in_ref.shape
    nq, tall, _ = p_ref.shape
    hidden = w_ref.shape[1]
    step = hidden // nq
    proj = tall - step
    x = in_ref[...].astype(F32).reshape(nz * rows, lanes).T
    at = hidden + proj
    fit = x[at : at + 1] + (x[at + 1 : at + 2] + x[at + 2 : at + 3])
    b = x[:hidden]
    weighted = (b * fit).astype(BF16)
    for g in range(w_ref.shape[0]):
        w_ref[g] = weighted
    b = b.astype(BF16)
    extra = x[hidden:at].astype(BF16)
    for q in range(nq):
        p_ref[q, :step] = b[q * step : (q + 1) * step]
        p_ref[q, step:] = extra


def base_rows(weight_ref, win_ref, out_ref):
    tok = win_ref.shape[0]
    spread = jnp.concatenate([win_ref[...]] * (LANE // tok), axis=0)
    out_ref[...] = lax.dot_general(weight_ref[...], spread, NT, preferred_element_type=F32)


def perturb(scale, in_ref, base_ref, out_ref):
    nq, tall, lanes = in_ref.shape
    own = base_ref.shape[0]
    step = up8(own)
    tok = (tall - step) // PARTS
    rank = 4
    wide = nq * lanes
    x = jnp.concatenate([in_ref[q] for q in range(nq)], axis=1)
    source = lax.broadcasted_iota(jnp.int32, (wide, wide), 0)
    target = lax.broadcasted_iota(jnp.int32, (wide, wide), 1)
    place = ((source & 127) >> 3) * 32 + (source >> 7) * 8 + (source & 7)
    move = jnp.where(place == target, 1.0, 0.0).astype(BF16)
    x = jnp.dot(x, move, preferred_element_type=F32)
    cands = LANE // rank
    n = lax.broadcasted_iota(jnp.int32, (cands * tok, PARTS * LANE), 0)
    k = lax.broadcasted_iota(jnp.int32, (cands * tok, PARTS * LANE), 1)
    same = (n // tok) == ((k & 127) >> 2)
    base = jnp.concatenate([base_ref[...]] * (cands * tok // LANE), axis=1)
    for part in range(wide // LANE):
        tile = x[:, part * LANE : (part + 1) * LANE]
        b = tile[:step].astype(BF16)
        left = jnp.concatenate([b] * PARTS, axis=1)
        proj = jnp.concatenate(
            [tile[step + i * tok : step + (i + 1) * tok] for i in range(PARTS)], axis=1
        )
        right = jnp.where(same, jnp.concatenate([proj] * cands, axis=0), 0.0).astype(BF16)
        low = lax.dot_general(left, right, NT, preferred_element_type=F32)
        out = base + scale * low[:own]
        out_ref[:, part * cands * tok : (part + 1) * cands * tok] = out.astype(BF16)


OFFSETS = ((0, 5, -5), (1, 6, -4), (-1, 4, -6), (2, 7, -3), (-2, 3, -7))


def update_parts(*refs):
    at_ref, w_ref = refs[:2]
    chunks, (first_ref, second_ref) = refs[2:7], refs[7:9]
    out_refs = refs[9:13]
    rows_ref, sum_ref = refs[13:]
    groups, nz, rows, width = rows_ref.shape
    z = at_ref[0]
    for ref, offsets in zip(chunks, OFFSETS):
        for i, offset in enumerate(offsets):
            place = lax.rem(z + offset + nz, nz)
            for g in range(groups):
                rows_ref[g, place] = ref[i, g]
    place = lax.rem(z + nz // 2, nz)
    for g in range(groups // 2):
        rows_ref[g, place] = first_ref[g]
        rows_ref[groups // 2 + g, place] = second_ref[g]
    left = jnp.concatenate([w_ref[g] for g in range(groups)], axis=1)
    right = rows_ref[...].reshape(groups * nz * rows, width)
    sum_ref[...] = jnp.dot(left, right, preferred_element_type=F32)
    y, core = at_ref[1], at_ref[2]
    tall = out_refs[0].shape[0]
    for ref, yy, cc in zip(out_refs, (y, y, 1 - y, 1 - y), (core, 1 - core, core, 1 - core)):
        start = pl.multiple_of((yy * 2 + cc) * tall, 8)
        ref[...] = sum_ref[pl.ds(start, tall), :]


def shifted(value, offset):
    n = lax.axis_size("z")
    return lax.ppermute(value, "z", [(i, (i - offset) % n) for i in range(n)])


def swapped(value, axis):
    return lax.ppermute(value, axis, [(0, 1), (1, 0)])


def local(window, weight, factor_a, factor_b, fitness):
    tok, depth = window.shape
    own = weight.shape[0]
    cands, rank, hidden = factor_b.shape
    groups, nz = lax.axis_size("grp"), lax.axis_size("z")
    nq = 4
    total = cands * groups * nz * nq
    rows = cands * rank
    width = depth // groups
    step = up8(own)
    lanes = upl(nq * step + PARTS * tok + 3)
    shape = jax.ShapeDtypeStruct

    cut = call(cut_a, "cut_a", shape((groups, rows, width), BF16), (factor_a,), 1 << 20)
    mine = lax.all_to_all(cut, "grp", 0, 0, tiled=True)

    packed = call(
        pack_b,
        "pack_b",
        shape((nz, rows, lanes), BF16),
        (fitness, window, factor_a, factor_b),
        1 << 24,
        scratch=[pltpu.VMEM((rows, upl(hidden) + 2 * LANE), F32)],
        smem=(0,),
    )
    columns = lax.all_to_all(packed, "z", 0, 0, tiled=True)
    weighted, pieces = call(
        turn_b,
        "turn_b",
        [
            shape((groups, nq * step, nz * rows), BF16),
            shape((nq, step + PARTS * tok, nz * rows), BF16),
        ],
        (columns,),
        1 << 24,
    )
    weighted = lax.all_to_all(weighted, "grp", 0, 0, tiled=True)
    pieces = lax.all_to_all(pieces, Q, 0, 0, tiled=True)
    base = call(base_rows, "base_rows", shape((own, LANE), F32), (weight, window), 1 << 28)
    perturbed = call(
        functools.partial(perturb, 0.25 / math.sqrt(depth)),
        "perturb",
        shape((own, cands * nz * nq * tok), BF16),
        (pieces, base),
        1 << 30,
    )

    mine = mine[None]
    near = jnp.concatenate([mine, shifted(mine, 5), shifted(mine, -5)], axis=0)
    up, down = shifted(near, 1), shifted(near, -1)
    up2, down2 = shifted(up, 1), shifted(down, -1)
    half = groups // 2
    first = shifted(up[1, :half], 2)
    second = shifted(down[2, half:], -2)
    at = jnp.stack([lax.axis_index("z"), lax.axis_index("yhi"), lax.axis_index("core")])
    part = shape((step, width), F32)
    oo, ox, xo, xx = call(
        update_parts,
        "update_parts",
        [part] * 4,
        (at.astype(jnp.int32), weighted, near, up, down, up2, down2, first, second),
        1 << 30,
        scratch=[
            pltpu.VMEM((groups, nz, rows, width), BF16),
            pltpu.VMEM((nq * step, width), F32),
        ],
        smem=(0,),
    )
    there = xo + swapped(xx, "core")
    here = oo + swapped(ox, "core")
    update = (here + swapped(there, "yhi"))[:own] * (0.5 / math.sqrt(total))
    return perturbed, update


def solution(mesh):
    split = Mesh(
        mesh.devices.reshape(mesh.shape["grp"], mesh.shape["shard"] // 4, 2, 2), GRP_SHARD
    )
    return jax.shard_map(
        local,
        mesh=split,
        in_specs=(
            P("grp", None),
            P(SHARD, None),
            P(GRP_SHARD, None, None),
            P(GRP_SHARD, None, None),
            P(GRP_SHARD),
        ),
        out_specs=(P(SHARD, "grp"), P(SHARD, "grp")),
        check_vma=False,
    )
```

```python
import functools
import math

import jax
import jax.numpy as jnp
from jax import lax
from jax.experimental import pallas as pl
from jax.experimental.pallas import tpu as pltpu
from jax.sharding import Mesh
from jax.sharding import PartitionSpec as P


F32, BF16 = jnp.float32, jnp.bfloat16
Q = ("yhi", "core")
SHARD = ("z", "yhi", "core")
GRP_SHARD = ("grp", "z", "yhi", "core")
LANE = 128
PARTS = 3
NT = (((1,), (1,)), ((), ()))


def up8(n):
    return (n + 7) // 8 * 8


def upl(n):
    return (n + LANE - 1) // LANE * LANE


def call(body, out_shape, args, flops, scratch=(), smem=()):
    vmem = pl.BlockSpec(memory_space=pltpu.VMEM)
    scalar = pl.BlockSpec(memory_space=pltpu.SMEM)
    many = isinstance(out_shape, (list, tuple))
    return pl.pallas_call(
        body,
        out_shape=out_shape,
        in_specs=[scalar if i in smem else vmem for i in range(len(args))],
        out_specs=[vmem] * len(out_shape) if many else vmem,
        scratch_shapes=list(scratch),
        cost_estimate=pl.CostEstimate(flops=flops, bytes_accessed=1 << 20, transcendentals=0),
        compiler_params=pltpu.CompilerParams(vmem_limit_bytes=40 << 20),
    )(*args)


def split3(x):
    hi = x.astype(BF16).astype(F32)
    rest = x - hi
    mid = rest.astype(BF16).astype(F32)
    return hi, mid, (rest - mid).astype(BF16).astype(F32)


def cut_a(a_ref, out_ref):
    groups, _, width = out_ref.shape
    cands = a_ref.shape[0]
    for g in range(groups):
        columns = slice(g * width, (g + 1) * width)
        both = [a_ref[c, :, columns].astype(F32) for c in range(cands)]
        out_ref[g] = jnp.concatenate(both, axis=0).astype(BF16)


def pack_b(fit_ref, win_ref, a_ref, b_ref, out_ref, wide_ref):
    nz, rows, lanes = out_ref.shape
    cands, rank, hidden = b_ref.shape
    tok, depth = win_ref.shape
    nq = 4
    own = hidden // (nz * nq)
    step = up8(own)
    for c in range(cands):
        wide_ref[c * rank : (c + 1) * rank, :hidden] = b_ref[c].astype(F32)
    wide_ref[:, hidden:] = jnp.zeros((rows, wide_ref.shape[1] - hidden), F32)
    a_rows = jnp.concatenate([a_ref[c].astype(F32) for c in range(cands)], axis=0).astype(BF16)
    first = nq * step % LANE
    win = win_ref[...]
    spread = jnp.concatenate(
        [jnp.zeros((first, depth), BF16)]
        + [win] * PARTS
        + [jnp.zeros((LANE - first - PARTS * tok, depth), BF16)],
        axis=0,
    )
    proj = lax.dot_general(a_rows, spread, NT, preferred_element_type=F32)
    lane = lax.broadcasted_iota(jnp.int32, (rows, LANE), 1)
    row = lax.broadcasted_iota(jnp.int32, (rows, LANE), 0)
    hi, mid, lo = split3(proj)
    extra = jnp.where(lane < first + tok, hi, jnp.where(lane < first + 2 * tok, mid, lo))
    fit = jnp.where(row < rank, fit_ref[0], fit_ref[1])
    fhi, fmid, flo = split3(fit)
    at = first + PARTS * tok
    fits = jnp.where(lane == at, fhi, jnp.where(lane == at + 1, fmid, flo))
    extra = jnp.where(lane < at, extra, jnp.where(lane < at + 3, fits, 0.0))
    for z in range(nz):
        block = [jnp.zeros((rows, LANE), F32) for _ in range(lanes // LANE)]
        for q in range(nq):
            source = (z * nq + q) * own
            base = source // LANE * LANE
            target = q * step
            start = target // LANE
            offset = target % LANE
            span = min(3, len(block) - start)
            window = wide_ref[:, base : base + 3 * LANE]
            turn = (offset - (source - base)) % (3 * LANE)
            if turn:
                window = pltpu.roll(window, turn, 1)
            for k in range(span):
                at_lane = lane + k * LANE
                inside = (at_lane >= offset) & (at_lane < offset + own)
                piece = window[:, k * LANE : (k + 1) * LANE]
                block[start + k] = jnp.where(inside, piece, block[start + k])
        block[-1] = jnp.where(lane >= first, extra, block[-1])
        out_ref[z] = jnp.concatenate(block, axis=1).astype(BF16)


def turn_b(in_ref, w_ref, p_ref):
    nz, rows, lanes = in_ref.shape
    nq, tall, _ = p_ref.shape
    hidden = w_ref.shape[1]
    step = hidden // nq
    proj = tall - step
    x = in_ref[...].astype(F32).reshape(nz * rows, lanes).T
    at = hidden + proj
    fit = x[at : at + 1] + (x[at + 1 : at + 2] + x[at + 2 : at + 3])
    b = x[:hidden]
    weighted = (b * fit).astype(BF16)
    for g in range(w_ref.shape[0]):
        w_ref[g] = weighted
    b = b.astype(BF16)
    extra = x[hidden:at].astype(BF16)
    for q in range(nq):
        p_ref[q, :step] = b[q * step : (q + 1) * step]
        p_ref[q, step:] = extra


def base_rows(weight_ref, win_ref, out_ref):
    tok = win_ref.shape[0]
    spread = jnp.concatenate([win_ref[...]] * (LANE // tok), axis=0)
    out_ref[...] = lax.dot_general(weight_ref[...], spread, NT, preferred_element_type=F32)


def perturb(scale, in_ref, base_ref, out_ref):
    nq, tall, lanes = in_ref.shape
    own = base_ref.shape[0]
    step = up8(own)
    tok = (tall - step) // PARTS
    rank = 4
    wide = nq * lanes
    x = jnp.concatenate([in_ref[q] for q in range(nq)], axis=1)
    source = lax.broadcasted_iota(jnp.int32, (wide, wide), 0)
    target = lax.broadcasted_iota(jnp.int32, (wide, wide), 1)
    place = ((source & 127) >> 3) * 32 + (source >> 7) * 8 + (source & 7)
    move = jnp.where(place == target, 1.0, 0.0).astype(BF16)
    x = jnp.dot(x, move, preferred_element_type=F32)
    cands = LANE // rank
    n = lax.broadcasted_iota(jnp.int32, (cands * tok, PARTS * LANE), 0)
    k = lax.broadcasted_iota(jnp.int32, (cands * tok, PARTS * LANE), 1)
    same = (n // tok) == ((k & 127) >> 2)
    base = jnp.concatenate([base_ref[...]] * (cands * tok // LANE), axis=1)
    for part in range(wide // LANE):
        tile = x[:, part * LANE : (part + 1) * LANE]
        b = tile[:step].astype(BF16)
        left = jnp.concatenate([b] * PARTS, axis=1)
        proj = jnp.concatenate(
            [tile[step + i * tok : step + (i + 1) * tok] for i in range(PARTS)], axis=1
        )
        right = jnp.where(same, jnp.concatenate([proj] * cands, axis=0), 0.0).astype(BF16)
        low = lax.dot_general(left, right, NT, preferred_element_type=F32)
        out = base + scale * low[:own]
        out_ref[:, part * cands * tok : (part + 1) * cands * tok] = out.astype(BF16)


OFFSETS = ((0, 5, -5), (1, 6, -4), (-1, 4, -6), (2, 7, -3), (-2, 3, -7))


def update_parts(*refs):
    at_ref, w_ref = refs[:2]
    chunks, (first_ref, second_ref) = refs[2:7], refs[7:9]
    out_refs = refs[9:13]
    rows_ref, sum_ref = refs[13:]
    groups, nz, rows, width = rows_ref.shape
    z = at_ref[0]
    for ref, offsets in zip(chunks, OFFSETS):
        for i, offset in enumerate(offsets):
            place = lax.rem(z + offset + nz, nz)
            for g in range(groups):
                rows_ref[g, place] = ref[i, g]
    place = lax.rem(z + nz // 2, nz)
    for g in range(groups // 2):
        rows_ref[g, place] = first_ref[g]
        rows_ref[groups // 2 + g, place] = second_ref[g]
    left = jnp.concatenate([w_ref[g] for g in range(groups)], axis=1)
    right = rows_ref[...].reshape(groups * nz * rows, width)
    sum_ref[...] = jnp.dot(left, right, preferred_element_type=F32)
    y, core = at_ref[1], at_ref[2]
    tall = out_refs[0].shape[0]
    for ref, yy, cc in zip(out_refs, (y, y, 1 - y, 1 - y), (core, 1 - core, core, 1 - core)):
        start = pl.multiple_of((yy * 2 + cc) * tall, 8)
        ref[...] = sum_ref[pl.ds(start, tall), :]


def shifted(value, offset):
    n = lax.axis_size("z")
    return lax.ppermute(value, "z", [(i, (i - offset) % n) for i in range(n)])


def swapped(value, axis):
    return lax.ppermute(value, axis, [(0, 1), (1, 0)])


def exchanged(value, axis):
    return lax.all_to_all(value, axis, 0, 0, tiled=True)


def step(window, weight, factor_a, factor_b, fitness):
    tok, depth = window.shape
    own = weight.shape[0]
    cands, rank, hidden = factor_b.shape
    groups, nz = lax.axis_size("grp"), lax.axis_size("z")
    nq = 4
    total = cands * groups * nz * nq
    rows = cands * rank
    width = depth // groups
    block = up8(own)
    lanes = upl(nq * block + PARTS * tok + 3)
    shape = jax.ShapeDtypeStruct

    cut = call(cut_a, shape((groups, rows, width), BF16), (factor_a,), 1 << 20)
    mine = exchanged(cut, "grp")

    packed = call(
        pack_b,
        shape((nz, rows, lanes), BF16),
        (fitness, window, factor_a, factor_b),
        1 << 24,
        scratch=[pltpu.VMEM((rows, upl(hidden) + 2 * LANE), F32)],
        smem=(0,),
    )
    columns = exchanged(packed, "z")
    weighted, pieces = call(
        turn_b,
        [
            shape((groups, nq * block, nz * rows), BF16),
            shape((nq, block + PARTS * tok, nz * rows), BF16),
        ],
        (columns,),
        1 << 24,
    )
    weighted = exchanged(weighted, "grp")
    pieces = exchanged(pieces, Q)
    base = call(base_rows, shape((own, LANE), F32), (weight, window), 1 << 28)
    perturbed = call(
        functools.partial(perturb, 0.25 / math.sqrt(depth)),
        shape((own, cands * nz * nq * tok), BF16),
        (pieces, base),
        1 << 30,
    )

    mine = mine[None]
    near = jnp.concatenate([mine, shifted(mine, 5), shifted(mine, -5)], axis=0)
    up, down = shifted(near, 1), shifted(near, -1)
    up2, down2 = shifted(up, 1), shifted(down, -1)
    half = groups // 2
    first = shifted(up[1, :half], 2)
    second = shifted(down[2, half:], -2)
    at = jnp.stack([lax.axis_index("z"), lax.axis_index("yhi"), lax.axis_index("core")])
    part = shape((block, width), F32)
    oo, ox, xo, xx = call(
        update_parts,
        [part] * 4,
        (at.astype(jnp.int32), weighted, near, up, down, up2, down2, first, second),
        1 << 30,
        scratch=[
            pltpu.VMEM((groups, nz, rows, width), BF16),
            pltpu.VMEM((nq * block, width), F32),
        ],
        smem=(0,),
    )
    there = xo + swapped(xx, "core")
    here = oo + swapped(ox, "core")
    update = (here + swapped(there, "yhi"))[:own] * (0.5 / math.sqrt(total))
    return perturbed, update


def solution(mesh):
    split = Mesh(
        mesh.devices.reshape(mesh.shape["grp"], mesh.shape["shard"] // 4, 2, 2), GRP_SHARD
    )
    return jax.shard_map(
        step,
        mesh=split,
        in_specs=(
            P("grp", None),
            P(SHARD, None),
            P(GRP_SHARD, None, None),
            P(GRP_SHARD, None, None),
            P(GRP_SHARD),
        ),
        out_specs=(P(SHARD, "grp"), P(SHARD, "grp")),
        check_vma=False,
    )
```

```python
import functools
import math

import jax
import jax.numpy as jnp
from jax import lax
from jax.experimental import pallas as pl
from jax.experimental.pallas import tpu as pltpu
from jax.sharding import Mesh
from jax.sharding import PartitionSpec as P


F32, BF16 = jnp.float32, jnp.bfloat16
Q = ("yhi", "core")
SHARD = ("z", "yhi", "core")
GRP_SHARD = ("grp", "z", "yhi", "core")
LANE = 128
PARTS = 3
NT = (((1,), (1,)), ((), ()))


def up8(n):
    return (n + 7) // 8 * 8


def upl(n):
    return (n + LANE - 1) // LANE * LANE


def call(body, out_shape, args, flops, scratch=(), smem=()):
    vmem = pl.BlockSpec(memory_space=pltpu.VMEM)
    scalar = pl.BlockSpec(memory_space=pltpu.SMEM)
    many = isinstance(out_shape, (list, tuple))
    return pl.pallas_call(
        body,
        out_shape=out_shape,
        in_specs=[scalar if i in smem else vmem for i in range(len(args))],
        out_specs=[vmem] * len(out_shape) if many else vmem,
        scratch_shapes=list(scratch),
        cost_estimate=pl.CostEstimate(flops=flops, bytes_accessed=1 << 20, transcendentals=0),
        compiler_params=pltpu.CompilerParams(vmem_limit_bytes=16 << 20),
    )(*args)


def split3(x):
    hi = x.astype(BF16).astype(F32)
    rest = x - hi
    mid = rest.astype(BF16).astype(F32)
    return hi, mid, (rest - mid).astype(BF16).astype(F32)


def cut_a(a_ref, out_ref):
    groups, _, width = out_ref.shape
    cands = a_ref.shape[0]
    for g in range(groups):
        columns = slice(g * width, (g + 1) * width)
        both = [a_ref[c, :, columns].astype(F32) for c in range(cands)]
        out_ref[g] = jnp.concatenate(both, axis=0).astype(BF16)


def pack_b(fit_ref, win_ref, a_ref, b_ref, out_ref, wide_ref):
    nz, rows, lanes = out_ref.shape
    cands, rank, hidden = b_ref.shape
    tok, depth = win_ref.shape
    nq = 4
    own = hidden // (nz * nq)
    step = up8(own)
    for c in range(cands):
        wide_ref[c * rank : (c + 1) * rank, :hidden] = b_ref[c].astype(F32)
    wide_ref[:, hidden:] = jnp.zeros((rows, wide_ref.shape[1] - hidden), F32)
    a_rows = jnp.concatenate([a_ref[c].astype(F32) for c in range(cands)], axis=0).astype(BF16)
    first = nq * step % LANE
    win = win_ref[...]
    spread = jnp.concatenate(
        [jnp.zeros((first, depth), BF16)]
        + [win] * PARTS
        + [jnp.zeros((LANE - first - PARTS * tok, depth), BF16)],
        axis=0,
    )
    proj = lax.dot_general(a_rows, spread, NT, preferred_element_type=F32)
    lane = lax.broadcasted_iota(jnp.int32, (rows, LANE), 1)
    row = lax.broadcasted_iota(jnp.int32, (rows, LANE), 0)
    hi, mid, lo = split3(proj)
    extra = jnp.where(lane < first + tok, hi, jnp.where(lane < first + 2 * tok, mid, lo))
    fit = jnp.where(row < rank, fit_ref[0], fit_ref[1])
    fhi, fmid, flo = split3(fit)
    at = first + PARTS * tok
    fits = jnp.where(lane == at, fhi, jnp.where(lane == at + 1, fmid, flo))
    extra = jnp.where(lane < at, extra, jnp.where(lane < at + 3, fits, 0.0))
    for z in range(nz):
        block = [jnp.zeros((rows, LANE), F32) for _ in range(lanes // LANE)]
        for q in range(nq):
            source = (z * nq + q) * own
            base = source // LANE * LANE
            target = q * step
            start = target // LANE
            offset = target % LANE
            span = min(3, len(block) - start)
            window = wide_ref[:, base : base + 3 * LANE]
            turn = (offset - (source - base)) % (3 * LANE)
            if turn:
                window = pltpu.roll(window, turn, 1)
            for k in range(span):
                at_lane = lane + k * LANE
                inside = (at_lane >= offset) & (at_lane < offset + own)
                piece = window[:, k * LANE : (k + 1) * LANE]
                block[start + k] = jnp.where(inside, piece, block[start + k])
        block[-1] = jnp.where(lane >= first, extra, block[-1])
        out_ref[z] = jnp.concatenate(block, axis=1).astype(BF16)


def turn_b(in_ref, w_ref, *refs):
    p_refs, hold_ref = refs[:-1], refs[-1]
    nz, rows, lanes = in_ref.shape
    nq = len(p_refs)
    tall = p_refs[0].shape[0]
    hidden = w_ref.shape[1]
    block = hidden // nq
    proj = tall - block
    x = in_ref[...].astype(F32).reshape(nz * rows, lanes).T
    at = hidden + proj
    fit = x[at : at + 1] + (x[at + 1 : at + 2] + x[at + 2 : at + 3])
    b = x[:hidden]
    weighted = (b * fit).astype(BF16)
    for g in range(w_ref.shape[0]):
        w_ref[g] = weighted
    hold_ref[...] = b.astype(BF16)
    extra = x[hidden:at].astype(BF16)
    q = lax.axis_index("yhi") * 2 + lax.axis_index("core")
    for j, ref in enumerate(p_refs):
        start = pl.multiple_of((q ^ j) * block, 8)
        ref[:block] = hold_ref[pl.ds(start, block), :]
        ref[block:] = extra


def base_rows(weight_ref, win_ref, out_ref):
    tok = win_ref.shape[0]
    spread = jnp.concatenate([win_ref[...]] * (LANE // tok), axis=0)
    out_ref[...] = lax.dot_general(weight_ref[...], spread, NT, preferred_element_type=F32)


def perturb(scale, base_ref, *refs):
    in_refs, out_ref, hold_ref = refs[:-2], refs[-2], refs[-1]
    nq, tall, lanes = hold_ref.shape
    own_q = lax.axis_index("yhi") * 2 + lax.axis_index("core")
    for j, ref in enumerate(in_refs):
        hold_ref[own_q ^ j] = ref[...]
    own = base_ref.shape[0]
    step = up8(own)
    tok = (tall - step) // PARTS
    rank = 4
    wide = nq * lanes
    x = jnp.concatenate([hold_ref[q] for q in range(nq)], axis=1)
    source = lax.broadcasted_iota(jnp.int32, (wide, wide), 0)
    target = lax.broadcasted_iota(jnp.int32, (wide, wide), 1)
    place = ((source & 127) >> 3) * 32 + (source >> 7) * 8 + (source & 7)
    move = jnp.where(place == target, 1.0, 0.0).astype(BF16)
    x = jnp.dot(x, move, preferred_element_type=F32)
    cands = LANE // rank
    n = lax.broadcasted_iota(jnp.int32, (cands * tok, PARTS * LANE), 0)
    k = lax.broadcasted_iota(jnp.int32, (cands * tok, PARTS * LANE), 1)
    same = (n // tok) == ((k & 127) >> 2)
    base = jnp.concatenate([base_ref[...]] * (cands * tok // LANE), axis=1)
    for part in range(wide // LANE):
        tile = x[:, part * LANE : (part + 1) * LANE]
        b = tile[:step].astype(BF16)
        left = jnp.concatenate([b] * PARTS, axis=1)
        proj = jnp.concatenate(
            [tile[step + i * tok : step + (i + 1) * tok] for i in range(PARTS)], axis=1
        )
        right = jnp.where(same, jnp.concatenate([proj] * cands, axis=0), 0.0).astype(BF16)
        low = lax.dot_general(left, right, NT, preferred_element_type=F32)
        out = base + scale * low[:own]
        out_ref[:, part * cands * tok : (part + 1) * cands * tok] = out.astype(BF16)


OFFSETS = ((0, 5, -5), (1, 6, -4), (-1, 4, -6), (2, 7, -3), (-2, 3, -7), (8,))


def update_parts(*refs):
    w_ref, chunks, out_refs = refs[0], refs[1:7], refs[7:11]
    rows_ref, sum_ref = refs[11:]
    groups, nz, rows, width = rows_ref.shape
    z, y, core = (lax.axis_index(name) for name in SHARD)
    for ref, offsets in zip(chunks, OFFSETS):
        for i, offset in enumerate(offsets):
            place = lax.rem(z + offset + nz, nz)
            for g in range(groups):
                rows_ref[g, place] = ref[i, g]
    left = jnp.concatenate([w_ref[g] for g in range(groups)], axis=1)
    right = rows_ref[...].reshape(groups * nz * rows, width)
    sum_ref[...] = jnp.dot(left, right, preferred_element_type=F32)
    tall = out_refs[0].shape[0]
    for ref, yy, cc in zip(out_refs, (y, y, 1 - y, 1 - y), (core, 1 - core, core, 1 - core)):
        start = pl.multiple_of((yy * 2 + cc) * tall, 8)
        ref[...] = sum_ref[pl.ds(start, tall), :]


def shifted(value, offset):
    n = lax.axis_size("z")
    return lax.ppermute(value, "z", [(i, (i - offset) % n) for i in range(n)])


def swapped(value, axis):
    return lax.ppermute(value, axis, [(0, 1), (1, 0)])


def turned(value, j):
    return lax.ppermute(value, Q, [(q, q ^ j) for q in range(4)])


def exchanged(value, axis):
    return lax.all_to_all(value, axis, 0, 0, tiled=True)


def step(window, weight, factor_a, factor_b, fitness):
    tok, depth = window.shape
    own = weight.shape[0]
    cands, rank, hidden = factor_b.shape
    groups, nz = lax.axis_size("grp"), lax.axis_size("z")
    nq = 4
    total = cands * groups * nz * nq
    rows = cands * rank
    width = depth // groups
    block = up8(own)
    lanes = upl(nq * block + PARTS * tok + 3)
    shape = jax.ShapeDtypeStruct

    cut = call(cut_a, shape((groups, rows, width), BF16), (factor_a,), 1 << 20)
    mine = exchanged(cut, "grp")

    packed = call(
        pack_b,
        shape((nz, rows, lanes), BF16),
        (fitness, window, factor_a, factor_b),
        1 << 24,
        scratch=[pltpu.VMEM((rows, upl(hidden) + 2 * LANE), F32)],
        smem=(0,),
    )
    columns = exchanged(packed, "z")
    tall = block + PARTS * tok
    weighted, *pieces = call(
        turn_b,
        [shape((groups, nq * block, nz * rows), BF16)] + [shape((tall, nz * rows), BF16)] * nq,
        (columns,),
        1 << 24,
        scratch=[pltpu.VMEM((nq * block, nz * rows), BF16)],
    )
    weighted = exchanged(weighted, "grp")
    pieces[1:] = [turned(pieces[j], j) for j in range(1, nq)]
    base = call(base_rows, shape((own, LANE), F32), (weight, window), 1 << 28)
    perturbed = call(
        functools.partial(perturb, 0.25 / math.sqrt(depth)),
        shape((own, cands * nz * nq * tok), BF16),
        (base, *pieces),
        1 << 30,
        scratch=[pltpu.VMEM((nq, tall, nz * rows), BF16)],
    )

    mine = mine[None]
    far = shifted(mine, 5)
    near = jnp.concatenate([mine, far, shifted(mine, -5)], axis=0)
    up, down = shifted(near, 1), shifted(near, -1)
    up2, down2 = shifted(up, 1), shifted(down, -1)
    across = shifted(far, 3)
    part = shape((block, width), F32)
    oo, ox, xo, xx = call(
        update_parts,
        [part] * 4,
        (weighted, near, up, down, up2, down2, across),
        1 << 30,
        scratch=[
            pltpu.VMEM((groups, nz, rows, width), BF16),
            pltpu.VMEM((nq * block, width), F32),
        ],
    )
    there = xo + swapped(xx, "core")
    here = oo + swapped(ox, "core")
    update = (here + swapped(there, "yhi"))[:own] * (0.5 / math.sqrt(total))
    return perturbed, update


def solution(mesh):
    split = Mesh(
        mesh.devices.reshape(mesh.shape["grp"], mesh.shape["shard"] // 4, 2, 2), GRP_SHARD
    )
    return jax.shard_map(
        step,
        mesh=split,
        in_specs=(
            P("grp", None),
            P(SHARD, None),
            P(GRP_SHARD, None, None),
            P(GRP_SHARD, None, None),
            P(GRP_SHARD),
        ),
        out_specs=(P(SHARD, "grp"), P(SHARD, "grp")),
        check_vma=False,
    )
```

```python
import functools
import math

import jax
import jax.numpy as jnp
from jax import lax
from jax.experimental import pallas as pl
from jax.experimental.pallas import tpu as pltpu
from jax.sharding import Mesh
from jax.sharding import PartitionSpec as P


F32, BF16 = jnp.float32, jnp.bfloat16
SHARD = ("z", "yhi", "core")
GRP_SHARD = ("grp", "z", "yhi", "core")
LANE = 128
PARTS = 2
NT = (((1,), (1,)), ((), ()))


def up8(n):
    return (n + 7) // 8 * 8


def upl(n):
    return (n + LANE - 1) // LANE * LANE


def call(body, out_shape, args, flops, scratch=(), smem=()):
    vmem = pl.BlockSpec(memory_space=pltpu.VMEM)
    scalar = pl.BlockSpec(memory_space=pltpu.SMEM)
    many = isinstance(out_shape, (list, tuple))
    return pl.pallas_call(
        body,
        out_shape=out_shape,
        in_specs=[scalar if i in smem else vmem for i in range(len(args))],
        out_specs=[vmem] * len(out_shape) if many else vmem,
        scratch_shapes=list(scratch),
        cost_estimate=pl.CostEstimate(flops=flops, bytes_accessed=1 << 20, transcendentals=0),
        compiler_params=pltpu.CompilerParams(vmem_limit_bytes=16 << 20),
    )(*args)


def split3(x):
    hi = x.astype(BF16).astype(F32)
    rest = x - hi
    mid = rest.astype(BF16).astype(F32)
    return hi, mid, (rest - mid).astype(BF16).astype(F32)


def cut_a(a_ref, out_ref):
    groups, _, width = out_ref.shape
    cands = a_ref.shape[0]
    for g in range(groups):
        columns = slice(g * width, (g + 1) * width)
        both = [a_ref[c, :, columns].astype(F32) for c in range(cands)]
        out_ref[g] = jnp.concatenate(both, axis=0).astype(BF16)


def layout(own, tok):
    first = up8(own)
    second = first + PARTS * tok
    return first, second, second + own, upl(second + own + 3)


def pack_b(fit_ref, win_ref, a_ref, b_ref, out_ref, wide_ref):
    blocks, rows, lanes = out_ref.shape
    cands, rank, hidden = b_ref.shape
    tok, depth = win_ref.shape
    own = hidden // (2 * blocks)
    proj_at, second, fit_at, _ = layout(own, tok)
    for c in range(cands):
        wide_ref[c * rank : (c + 1) * rank, :hidden] = b_ref[c].astype(F32)
    wide_ref[:, hidden:] = jnp.zeros((rows, wide_ref.shape[1] - hidden), F32)
    a_rows = jnp.concatenate([a_ref[c].astype(F32) for c in range(cands)], axis=0).astype(BF16)
    first = proj_at % LANE
    win = win_ref[...]
    spread = jnp.concatenate(
        [jnp.zeros((first, depth), BF16)]
        + [win] * PARTS
        + [jnp.zeros((LANE - first - PARTS * tok, depth), BF16)],
        axis=0,
    )
    proj = lax.dot_general(a_rows, spread, NT, preferred_element_type=F32)
    lane = lax.broadcasted_iota(jnp.int32, (rows, LANE), 1)
    row = lax.broadcasted_iota(jnp.int32, (rows, LANE), 0)
    high, mid, _ = split3(proj)
    extra = jnp.where(lane < first + tok, high, mid)
    has_extra = (lane >= first) & (lane < first + PARTS * tok)
    fit = jnp.where(row < rank, fit_ref[0], fit_ref[1])
    fits = split3(fit)
    at = fit_at % LANE
    for z in range(blocks // 2):
        for core in range(2):
            block = [jnp.zeros((rows, LANE), F32) for _ in range(lanes // LANE)]
            for y in range(2):
                source = ((z * 2 + y) * 2 + core) * own
                base = source // LANE * LANE
                target = y * second
                start = target // LANE
                offset = target % LANE
                span = min(3, len(block) - start)
                window = wide_ref[:, base : base + 3 * LANE]
                turn = (offset - (source - base)) % (3 * LANE)
                if turn:
                    window = pltpu.roll(window, turn, 1)
                for k in range(span):
                    at_lane = lane + k * LANE
                    inside = (at_lane >= offset) & (at_lane < offset + own)
                    piece = window[:, k * LANE : (k + 1) * LANE]
                    block[start + k] = jnp.where(inside, piece, block[start + k])
            place = proj_at // LANE
            block[place] = jnp.where(has_extra, extra, block[place])
            place = fit_at // LANE
            for i, value in enumerate(fits):
                block[place] = jnp.where(lane == at + i, value, block[place])
            out_ref[z * 2 + core] = jnp.concatenate(block, axis=1).astype(BF16)


def turn_b(own, tok, in_ref, w_ref, keep_ref, send_ref, hold_ref):
    blocks, rows, lanes = in_ref.shape
    proj_at, second, fit_at, _ = layout(own, tok)
    block = proj_at
    wide = blocks * rows // 2
    x = in_ref[...].astype(F32).reshape(blocks // 2, 2, rows, lanes)
    for core in range(2):
        part = x[:, core].reshape(wide, lanes).T
        fit = part[fit_at : fit_at + 1] + (
            part[fit_at + 1 : fit_at + 2] + part[fit_at + 2 : fit_at + 3]
        )
        for y in range(2):
            b = part[y * second : y * second + block]
            weighted = (b * fit).astype(BF16)
            for g in range(w_ref.shape[0] // 2):
                w_ref[2 * g + core, y * block : (y + 1) * block] = weighted
            across = slice(core * wide, (core + 1) * wide)
            hold_ref[y, :block, across] = b.astype(BF16)
            hold_ref[y, block:, across] = part[proj_at:second].astype(BF16)
    y = lax.axis_index("yhi")
    keep_ref[...] = hold_ref[y]
    send_ref[...] = hold_ref[1 - y]


def base_rows(weight_ref, win_ref, out_ref):
    tok = win_ref.shape[0]
    spread = jnp.concatenate([win_ref[...]] * (LANE // tok), axis=0)
    out_ref[...] = lax.dot_general(weight_ref[...], spread, NT, preferred_element_type=F32)


def perturb(scale, base_ref, keep_ref, got_ref, out_ref, hold_ref):
    tall = keep_ref.shape[0]
    own_y = lax.axis_index("yhi")
    hold_ref[own_y] = keep_ref[...]
    hold_ref[1 - own_y] = got_ref[...]
    own = base_ref.shape[0]
    step = up8(own)
    tok = (tall - step) // PARTS
    rank = 4
    x = jnp.concatenate([hold_ref[0], hold_ref[1]], axis=1)
    wide = x.shape[1]
    source = lax.broadcasted_iota(jnp.int32, (wide, wide), 0)
    target = lax.broadcasted_iota(jnp.int32, (wide, wide), 1)
    place = ((source & 127) >> 3) * 32 + (source >> 7) * 8 + (source & 7)
    move = jnp.where(place == target, 1.0, 0.0).astype(BF16)
    x = jnp.dot(x, move, preferred_element_type=F32)
    cands = LANE // rank
    n = lax.broadcasted_iota(jnp.int32, (cands * tok, PARTS * LANE), 0)
    k = lax.broadcasted_iota(jnp.int32, (cands * tok, PARTS * LANE), 1)
    same = (n // tok) == ((k & 127) >> 2)
    base = jnp.concatenate([base_ref[...]] * (cands * tok // LANE), axis=1)
    for part in range(wide // LANE):
        tile = x[:, part * LANE : (part + 1) * LANE]
        b = tile[:step].astype(BF16)
        left = jnp.concatenate([b] * PARTS, axis=1)
        proj = jnp.concatenate(
            [tile[step + i * tok : step + (i + 1) * tok] for i in range(PARTS)], axis=1
        )
        right = jnp.where(same, jnp.concatenate([proj] * cands, axis=0), 0.0).astype(BF16)
        low = lax.dot_general(left, right, NT, preferred_element_type=F32)
        out = base + scale * low[:own]
        out_ref[:, part * cands * tok : (part + 1) * cands * tok] = out.astype(BF16)


OFFSETS = ((0, 5, -5), (1, 6, -4), (-1, 4, -6), (2, 7, -3), (-2, 3, -7), (8,))


def update_parts(*refs):
    w_ref, chunks, out_refs = refs[0], refs[1:7], refs[7:11]
    rows_ref, sum_ref = refs[11:]
    groups, nz, rows, width = rows_ref.shape
    z, y, core = (lax.axis_index(name) for name in SHARD)
    for ref, offsets in zip(chunks, OFFSETS):
        for i, offset in enumerate(offsets):
            place = lax.rem(z + offset + nz, nz)
            for g in range(groups):
                rows_ref[g, place] = ref[i, g]
    left = jnp.concatenate(
        [jnp.concatenate([w_ref[2 * g + c] for g in range(groups)], axis=1) for c in range(2)], axis=0
    )
    right = rows_ref[...].reshape(groups * nz * rows, width)
    sum_ref[...] = jnp.dot(left, right, preferred_element_type=F32)
    tall = out_refs[0].shape[0]
    for ref, yy, cc in zip(out_refs, (y, y, 1 - y, 1 - y), (core, 1 - core, core, 1 - core)):
        start = pl.multiple_of((cc * 2 + yy) * tall, 8)
        ref[...] = sum_ref[pl.ds(start, tall), :]


def shifted(value, offset):
    n = lax.axis_size("z")
    return lax.ppermute(value, "z", [(i, (i - offset) % n) for i in range(n)])


def swapped(value, axis):
    return lax.ppermute(value, axis, [(0, 1), (1, 0)])


def exchanged(value, axis):
    return lax.all_to_all(value, axis, 0, 0, tiled=True)


def step(window, weight, factor_a, factor_b, fitness):
    tok, depth = window.shape
    own = weight.shape[0]
    cands, rank, hidden = factor_b.shape
    groups, nz = lax.axis_size("grp"), lax.axis_size("z")
    nq = 4
    total = cands * groups * nz * nq
    rows = cands * rank
    width = depth // groups
    block = up8(own)
    tall = block + PARTS * tok
    shape = jax.ShapeDtypeStruct

    cut = call(cut_a, shape((groups, rows, width), BF16), (factor_a,), 1 << 20)
    mine = exchanged(cut, "grp")

    packed = call(
        pack_b,
        shape((nz * 2, rows, layout(own, tok)[-1]), BF16),
        (fitness, window, factor_a, factor_b),
        1 << 24,
        scratch=[pltpu.VMEM((rows, upl(hidden) + 2 * LANE), F32)],
        smem=(0,),
    )
    columns = exchanged(packed, ("z", "core"))
    weighted, keep, send = call(
        functools.partial(turn_b, own, tok),
        [
            shape((groups * 2, 2 * block, nz * rows), BF16),
            shape((tall, 2 * nz * rows), BF16),
            shape((tall, 2 * nz * rows), BF16),
        ],
        (columns,),
        1 << 24,
        scratch=[pltpu.VMEM((2, tall, 2 * nz * rows), BF16)],
    )
    weighted = exchanged(weighted, ("grp", "core"))
    got = swapped(send, "yhi")
    base = call(base_rows, shape((own, LANE), F32), (weight, window), 1 << 28)
    perturbed = call(
        functools.partial(perturb, 0.25 / math.sqrt(depth)),
        shape((own, cands * nz * nq * tok), BF16),
        (base, keep, got),
        1 << 30,
        scratch=[pltpu.VMEM((2, tall, 2 * nz * rows), BF16)],
    )

    mine = mine[None]
    far = shifted(mine, 5)
    near = jnp.concatenate([mine, far, shifted(mine, -5)], axis=0)
    up, down = shifted(near, 1), shifted(near, -1)
    up2, down2 = shifted(up, 1), shifted(down, -1)
    across = shifted(far, 3)
    part = shape((block, width), F32)
    oo, ox, xo, xx = call(
        update_parts,
        [part] * 4,
        (weighted, near, up, down, up2, down2, across),
        1 << 30,
        scratch=[
            pltpu.VMEM((groups, nz, rows, width), BF16),
            pltpu.VMEM((nq * block, width), F32),
        ],
    )
    there = xo + swapped(xx, "core")
    here = oo + swapped(ox, "core")
    update = (here + swapped(there, "yhi"))[:own] * (0.5 / math.sqrt(total))
    return perturbed, update


def solution(mesh):
    split = Mesh(
        mesh.devices.reshape(mesh.shape["grp"], mesh.shape["shard"] // 4, 2, 2), GRP_SHARD
    )
    return jax.shard_map(
        step,
        mesh=split,
        in_specs=(
            P("grp", None),
            P(SHARD, None),
            P(GRP_SHARD, None, None),
            P(GRP_SHARD, None, None),
            P(GRP_SHARD),
        ),
        out_specs=(P(SHARD, "grp"), P(SHARD, "grp")),
        check_vma=False,
    )
```

```python
import functools
import math

import jax
import jax.numpy as jnp
from jax import lax
from jax.experimental import pallas as pl
from jax.experimental.pallas import tpu as pltpu
from jax.sharding import Mesh
from jax.sharding import PartitionSpec as P


F32, BF16 = jnp.float32, jnp.bfloat16
SHARD = ("z", "yhi", "core")
GRP_SHARD = ("grp", "z", "yhi", "core")
LANE = 128
PARTS = 2
NT = (((1,), (1,)), ((), ()))


def up8(n):
    return (n + 7) // 8 * 8


def upl(n):
    return (n + LANE - 1) // LANE * LANE


def call(body, out_shape, args, flops, scratch=(), smem=(), far=()):
    vmem = pl.BlockSpec(memory_space=pltpu.VMEM)
    scalar = pl.BlockSpec(memory_space=pltpu.SMEM)
    many = isinstance(out_shape, (list, tuple))
    return pl.pallas_call(
        body,
        out_shape=out_shape,
        in_specs=[
            scalar if i in smem else pl.BlockSpec(memory_space=pltpu.HBM) if i in far else vmem
            for i in range(len(args))
        ],
        out_specs=[vmem] * len(out_shape) if many else vmem,
        scratch_shapes=list(scratch),
        cost_estimate=pl.CostEstimate(flops=flops, bytes_accessed=1 << 20, transcendentals=0),
        compiler_params=pltpu.CompilerParams(vmem_limit_bytes=(60 if far else 16) << 20),
    )(*args)


def split3(x):
    hi = x.astype(BF16).astype(F32)
    rest = x - hi
    mid = rest.astype(BF16).astype(F32)
    return hi, mid, (rest - mid).astype(BF16).astype(F32)


def cut_a(a_hbm, out_ref, a_ref, sem):
    load = pltpu.make_async_copy(a_hbm, a_ref, sem)
    load.start()
    load.wait()
    groups, _, width = out_ref.shape
    cands = a_ref.shape[0]
    for g in range(groups):
        columns = slice(g * width, (g + 1) * width)
        both = [a_ref[c, :, columns].astype(F32) for c in range(cands)]
        out_ref[g] = jnp.concatenate(both, axis=0).astype(BF16)


def layout(own, tok):
    first = up8(own)
    second = first + PARTS * tok
    return first, second, second + own, upl(second + own + 3)


def pack_b(fit_ref, win_hbm, a_hbm, b_hbm, out_ref, wide_ref, win_ref, a_ref, b_ref, sems):
    loads = [
        pltpu.make_async_copy(source, target, sems.at[i])
        for i, (source, target) in enumerate(
            ((b_hbm, b_ref), (a_hbm, a_ref), (win_hbm, win_ref))
        )
    ]
    for load in loads:
        load.start()
    for load in loads:
        load.wait()
    blocks, rows, lanes = out_ref.shape
    cands, rank, hidden = b_ref.shape
    tok, depth = win_ref.shape
    own = hidden // (2 * blocks)
    proj_at, second, fit_at, _ = layout(own, tok)
    for c in range(cands):
        wide_ref[c * rank : (c + 1) * rank, :hidden] = b_ref[c].astype(F32)
    wide_ref[:, hidden:] = jnp.zeros((rows, wide_ref.shape[1] - hidden), F32)
    a_rows = jnp.concatenate([a_ref[c].astype(F32) for c in range(cands)], axis=0).astype(BF16)
    first = proj_at % LANE
    win = win_ref[...]
    spread = jnp.concatenate(
        [jnp.zeros((first, depth), BF16)]
        + [win] * PARTS
        + [jnp.zeros((LANE - first - PARTS * tok, depth), BF16)],
        axis=0,
    )
    proj = lax.dot_general(a_rows, spread, NT, preferred_element_type=F32)
    lane = lax.broadcasted_iota(jnp.int32, (rows, LANE), 1)
    row = lax.broadcasted_iota(jnp.int32, (rows, LANE), 0)
    high, mid, _ = split3(proj)
    extra = jnp.where(lane < first + tok, high, mid)
    has_extra = (lane >= first) & (lane < first + PARTS * tok)
    fit = jnp.where(row < rank, fit_ref[0], fit_ref[1])
    fits = split3(fit)
    at = fit_at % LANE
    for z in range(blocks // 2):
        for core in range(2):
            block = [jnp.zeros((rows, LANE), F32) for _ in range(lanes // LANE)]
            for y in range(2):
                source = ((z * 2 + y) * 2 + core) * own
                base = source // LANE * LANE
                target = y * second
                start = target // LANE
                offset = target % LANE
                span = min(3, len(block) - start)
                window = wide_ref[:, base : base + 3 * LANE]
                turn = (offset - (source - base)) % (3 * LANE)
                if turn:
                    window = pltpu.roll(window, turn, 1)
                for k in range(span):
                    at_lane = lane + k * LANE
                    inside = (at_lane >= offset) & (at_lane < offset + own)
                    piece = window[:, k * LANE : (k + 1) * LANE]
                    block[start + k] = jnp.where(inside, piece, block[start + k])
            place = proj_at // LANE
            block[place] = jnp.where(has_extra, extra, block[place])
            place = fit_at // LANE
            for i, value in enumerate(fits):
                block[place] = jnp.where(lane == at + i, value, block[place])
            out_ref[z * 2 + core] = jnp.concatenate(block, axis=1).astype(BF16)


def turn_b(own, tok, in_ref, w_ref, keep_ref, send_ref, hold_ref):
    blocks, rows, lanes = in_ref.shape
    proj_at, second, fit_at, _ = layout(own, tok)
    block = proj_at
    wide = blocks * rows // 2
    x = in_ref[...].astype(F32).reshape(blocks // 2, 2, rows, lanes)
    for core in range(2):
        part = x[:, core].reshape(wide, lanes).T
        fit = part[fit_at : fit_at + 1] + (
            part[fit_at + 1 : fit_at + 2] + part[fit_at + 2 : fit_at + 3]
        )
        for y in range(2):
            b = part[y * second : y * second + block]
            weighted = (b * fit).astype(BF16)
            for g in range(w_ref.shape[0] // 2):
                w_ref[2 * g + core, y * block : (y + 1) * block] = weighted
            across = slice(core * wide, (core + 1) * wide)
            hold_ref[y, :block, across] = b.astype(BF16)
            hold_ref[y, block:, across] = part[proj_at:second].astype(BF16)
    y = lax.axis_index("yhi")
    keep_ref[...] = hold_ref[y]
    send_ref[...] = hold_ref[1 - y]


def base_rows(weight_ref, win_ref, out_ref):
    tok = win_ref.shape[0]
    spread = jnp.concatenate([win_ref[...]] * (LANE // tok), axis=0)
    out_ref[...] = lax.dot_general(weight_ref[...], spread, NT, preferred_element_type=F32)


def perturb(scale, base_ref, keep_ref, got_ref, out_ref, hold_ref):
    tall = keep_ref.shape[0]
    own_y = lax.axis_index("yhi")
    hold_ref[own_y] = keep_ref[...]
    hold_ref[1 - own_y] = got_ref[...]
    own = base_ref.shape[0]
    step = up8(own)
    tok = (tall - step) // PARTS
    rank = 4
    x = jnp.concatenate([hold_ref[0], hold_ref[1]], axis=1)
    wide = x.shape[1]
    source = lax.broadcasted_iota(jnp.int32, (wide, wide), 0)
    target = lax.broadcasted_iota(jnp.int32, (wide, wide), 1)
    place = ((source & 127) >> 3) * 32 + (source >> 7) * 8 + (source & 7)
    move = jnp.where(place == target, 1.0, 0.0).astype(BF16)
    x = jnp.dot(x, move, preferred_element_type=F32)
    cands = LANE // rank
    n = lax.broadcasted_iota(jnp.int32, (cands * tok, PARTS * LANE), 0)
    k = lax.broadcasted_iota(jnp.int32, (cands * tok, PARTS * LANE), 1)
    same = (n // tok) == ((k & 127) >> 2)
    base = jnp.concatenate([base_ref[...]] * (cands * tok // LANE), axis=1)
    for part in range(wide // LANE):
        tile = x[:, part * LANE : (part + 1) * LANE]
        b = tile[:step].astype(BF16)
        left = jnp.concatenate([b] * PARTS, axis=1)
        proj = jnp.concatenate(
            [tile[step + i * tok : step + (i + 1) * tok] for i in range(PARTS)], axis=1
        )
        right = jnp.where(same, jnp.concatenate([proj] * cands, axis=0), 0.0).astype(BF16)
        low = lax.dot_general(left, right, NT, preferred_element_type=F32)
        out = base + scale * low[:own]
        out_ref[:, part * cands * tok : (part + 1) * cands * tok] = out.astype(BF16)


OFFSETS = ((0, 5, -5), (1, 6, -4), (-1, 4, -6), (2, 7, -3), (-2, 3, -7), (8,))


def place_rows(chunks, rows_ref):
    groups, nz, _, _ = rows_ref.shape
    z = lax.axis_index("z")
    for ref, offsets in zip(chunks, OFFSETS):
        for i, offset in enumerate(offsets):
            place = lax.rem(z + offset + nz, nz)
            for g in range(groups):
                rows_ref[g, place] = ref[i, g]


def update_first(w_ref, *refs):
    chunks, out_ref, rows_ref = refs[:6], refs[6], refs[7]
    groups, nz, rows, width = rows_ref.shape
    place_rows(chunks, rows_ref)
    y, core = lax.axis_index("yhi"), lax.axis_index("core")
    tall = out_ref.shape[0]
    start = pl.multiple_of((1 - y) * tall, 8)
    left = jnp.concatenate(
        [w_ref[2 * g + 1 - core, pl.ds(start, tall), :] for g in range(groups)], axis=1
    )
    right = rows_ref[...].reshape(groups * nz * rows, width)
    out_ref[...] = jnp.dot(left, right, preferred_element_type=F32)


def update_rest(w_ref, *refs):
    chunks, out_refs, rows_ref = refs[:6], refs[6:9], refs[9]
    groups, nz, rows, width = rows_ref.shape
    place_rows(chunks, rows_ref)
    y, core = lax.axis_index("yhi"), lax.axis_index("core")
    tall = out_refs[0].shape[0]
    right = rows_ref[...].reshape(groups * nz * rows, width)
    for ref, yy, cc in zip(out_refs, (1 - y, y, y), (core, core, 1 - core)):
        start = pl.multiple_of(yy * tall, 8)
        left = jnp.concatenate(
            [w_ref[2 * g + cc, pl.ds(start, tall), :] for g in range(groups)], axis=1
        )
        ref[...] = jnp.dot(left, right, preferred_element_type=F32)


def shifted(value, offset):
    n = lax.axis_size("z")
    return lax.ppermute(value, "z", [(i, (i - offset) % n) for i in range(n)])


def swapped(value, axis):
    return lax.ppermute(value, axis, [(0, 1), (1, 0)])


def exchanged(value, axis):
    return lax.all_to_all(value, axis, 0, 0, tiled=True)


def step(window, weight, factor_a, factor_b, fitness):
    tok, depth = window.shape
    own = weight.shape[0]
    cands, rank, hidden = factor_b.shape
    groups, nz = lax.axis_size("grp"), lax.axis_size("z")
    nq = 4
    total = cands * groups * nz * nq
    rows = cands * rank
    width = depth // groups
    block = up8(own)
    tall = block + PARTS * tok
    shape = jax.ShapeDtypeStruct

    cut = call(
        cut_a,
        shape((groups, rows, width), BF16),
        (factor_a,),
        1 << 20,
        scratch=[pltpu.VMEM(factor_a.shape, BF16), pltpu.SemaphoreType.DMA],
        far=(0,),
    )
    mine = exchanged(cut, "grp")

    packed = call(
        pack_b,
        shape((nz * 2, rows, layout(own, tok)[-1]), BF16),
        (fitness, window, factor_a, factor_b),
        1 << 24,
        scratch=[
            pltpu.VMEM((rows, upl(hidden) + 2 * LANE), F32),
            pltpu.VMEM(window.shape, BF16),
            pltpu.VMEM(factor_a.shape, BF16),
            pltpu.VMEM(factor_b.shape, BF16),
            pltpu.SemaphoreType.DMA((3,)),
        ],
        smem=(0,),
        far=(1, 2, 3),
    )
    columns = exchanged(packed, ("z", "core"))
    weighted, keep, send = call(
        functools.partial(turn_b, own, tok),
        [
            shape((groups * 2, 2 * block, nz * rows), BF16),
            shape((tall, 2 * nz * rows), BF16),
            shape((tall, 2 * nz * rows), BF16),
        ],
        (columns,),
        1 << 24,
        scratch=[pltpu.VMEM((2, tall, 2 * nz * rows), BF16)],
    )
    weighted = exchanged(weighted, ("grp", "core"))
    got = swapped(send, "yhi")
    base = call(base_rows, shape((own, LANE), F32), (weight, window), 1 << 28)
    perturbed = call(
        functools.partial(perturb, 0.25 / math.sqrt(depth)),
        shape((own, cands * nz * nq * tok), BF16),
        (base, keep, got),
        1 << 30,
        scratch=[pltpu.VMEM((2, tall, 2 * nz * rows), BF16)],
    )

    mine = mine[None]
    far = shifted(mine, 5)
    near = jnp.concatenate([mine, far, shifted(mine, -5)], axis=0)
    up, down = shifted(near, 1), shifted(near, -1)
    up2, down2 = shifted(up, 1), shifted(down, -1)
    across = shifted(far, 3)
    part = shape((block, width), F32)
    operands = (weighted, near, up, down, up2, down2, across)
    held = [pltpu.VMEM((groups, nz, rows, width), BF16)]
    xx = call(update_first, part, operands, 1 << 28, scratch=held)
    xo, oo, ox = call(update_rest, [part] * 3, operands, 1 << 29, scratch=held)
    there = xo + swapped(xx, "core")
    here = oo + swapped(ox, "core")
    update = (here + swapped(there, "yhi"))[:own] * (0.5 / math.sqrt(total))
    return perturbed, update


def solution(mesh):
    split = Mesh(
        mesh.devices.reshape(mesh.shape["grp"], mesh.shape["shard"] // 4, 2, 2), GRP_SHARD
    )
    return jax.shard_map(
        step,
        mesh=split,
        in_specs=(
            P("grp", None),
            P(SHARD, None),
            P(GRP_SHARD, None, None),
            P(GRP_SHARD, None, None),
            P(GRP_SHARD),
        ),
        out_specs=(P(SHARD, "grp"), P(SHARD, "grp")),
        check_vma=False,
    )
```

```python
import functools
import math

import jax
import jax.numpy as jnp
from jax import lax
from jax.experimental import pallas as pl
from jax.experimental.pallas import tpu as pltpu
from jax.sharding import Mesh
from jax.sharding import PartitionSpec as P


F32, BF16 = jnp.float32, jnp.bfloat16
SHARD = ("z", "yhi", "core")
GRP_SHARD = ("grp", "z", "yhi", "core")
LANE = 128
PARTS = 2
NT = (((1,), (1,)), ((), ()))


def up8(n):
    return (n + 7) // 8 * 8


def upl(n):
    return (n + LANE - 1) // LANE * LANE


def call(body, out_shape, args, flops, scratch=(), smem=(), far=()):
    vmem = pl.BlockSpec(memory_space=pltpu.VMEM)
    scalar = pl.BlockSpec(memory_space=pltpu.SMEM)
    many = isinstance(out_shape, (list, tuple))
    return pl.pallas_call(
        body,
        out_shape=out_shape,
        in_specs=[
            scalar if i in smem else pl.BlockSpec(memory_space=pltpu.HBM) if i in far else vmem
            for i in range(len(args))
        ],
        out_specs=[vmem] * len(out_shape) if many else vmem,
        scratch_shapes=list(scratch),
        cost_estimate=pl.CostEstimate(flops=flops, bytes_accessed=1 << 20, transcendentals=0),
        compiler_params=pltpu.CompilerParams(vmem_limit_bytes=(60 if far else 16) << 20),
    )(*args)


def split3(x):
    hi = x.astype(BF16).astype(F32)
    rest = x - hi
    mid = rest.astype(BF16).astype(F32)
    return hi, mid, (rest - mid).astype(BF16).astype(F32)


def cut_a(a_hbm, out_ref, a_ref, sem):
    load = pltpu.make_async_copy(a_hbm, a_ref, sem)
    load.start()
    load.wait()
    groups, _, width = out_ref.shape
    cands = a_ref.shape[0]
    for g in range(groups):
        columns = slice(g * width, (g + 1) * width)
        both = [a_ref[c, :, columns].astype(F32) for c in range(cands)]
        out_ref[g] = jnp.concatenate(both, axis=0).astype(BF16)


def layout(own, tok):
    first = up8(own)
    second = first + PARTS * tok
    return first, second, second + own, upl(second + own + 3)


def pack_b(fit_ref, win_hbm, a_hbm, b_hbm, out_ref, wide_ref, win_ref, a_ref, b_ref, sems):
    loads = [
        pltpu.make_async_copy(source, target, sems.at[i])
        for i, (source, target) in enumerate(
            ((b_hbm, b_ref), (a_hbm, a_ref), (win_hbm, win_ref))
        )
    ]
    for load in loads:
        load.start()
    for load in loads:
        load.wait()
    blocks, rows, lanes = out_ref.shape
    cands, rank, hidden = b_ref.shape
    tok, depth = win_ref.shape
    own = hidden // (2 * blocks)
    proj_at, second, fit_at, _ = layout(own, tok)
    for c in range(cands):
        wide_ref[c * rank : (c + 1) * rank, :hidden] = b_ref[c].astype(F32)
    wide_ref[:, hidden:] = jnp.zeros((rows, wide_ref.shape[1] - hidden), F32)
    a_rows = jnp.concatenate([a_ref[c].astype(F32) for c in range(cands)], axis=0).astype(BF16)
    first = proj_at % LANE
    win = win_ref[...]
    spread = jnp.concatenate(
        [jnp.zeros((first, depth), BF16)]
        + [win] * PARTS
        + [jnp.zeros((LANE - first - PARTS * tok, depth), BF16)],
        axis=0,
    )
    proj = lax.dot_general(a_rows, spread, NT, preferred_element_type=F32)
    lane = lax.broadcasted_iota(jnp.int32, (rows, LANE), 1)
    row = lax.broadcasted_iota(jnp.int32, (rows, LANE), 0)
    high, mid, _ = split3(proj)
    extra = jnp.where(lane < first + tok, high, mid)
    has_extra = (lane >= first) & (lane < first + PARTS * tok)
    fit = jnp.where(row < rank, fit_ref[0], fit_ref[1])
    fits = split3(fit)
    at = fit_at % LANE
    for z in range(blocks // 2):
        for core in range(2):
            block = [jnp.zeros((rows, LANE), F32) for _ in range(lanes // LANE)]
            for y in range(2):
                source = ((z * 2 + y) * 2 + core) * own
                base = source // LANE * LANE
                target = y * second
                start = target // LANE
                offset = target % LANE
                span = min(3, len(block) - start)
                window = wide_ref[:, base : base + 3 * LANE]
                turn = (offset - (source - base)) % (3 * LANE)
                if turn:
                    window = pltpu.roll(window, turn, 1)
                for k in range(span):
                    at_lane = lane + k * LANE
                    inside = (at_lane >= offset) & (at_lane < offset + own)
                    piece = window[:, k * LANE : (k + 1) * LANE]
                    block[start + k] = jnp.where(inside, piece, block[start + k])
            place = proj_at // LANE
            block[place] = jnp.where(has_extra, extra, block[place])
            place = fit_at // LANE
            for i, value in enumerate(fits):
                block[place] = jnp.where(lane == at + i, value, block[place])
            out_ref[z * 2 + core] = jnp.concatenate(block, axis=1).astype(BF16)


def turn_b(own, tok, in_ref, w_ref, keep_ref, send_ref, hold_ref):
    blocks, rows, lanes = in_ref.shape
    proj_at, second, fit_at, _ = layout(own, tok)
    block = proj_at
    wide = blocks * rows // 2
    x = in_ref[...].astype(F32).reshape(blocks // 2, 2, rows, lanes)
    for core in range(2):
        part = x[:, core].reshape(wide, lanes).T
        fit = part[fit_at : fit_at + 1] + (
            part[fit_at + 1 : fit_at + 2] + part[fit_at + 2 : fit_at + 3]
        )
        for y in range(2):
            b = part[y * second : y * second + block]
            weighted = (b * fit).astype(BF16)
            for g in range(w_ref.shape[0] // 2):
                w_ref[2 * g + core, y * block : (y + 1) * block] = weighted
            across = slice(core * wide, (core + 1) * wide)
            hold_ref[y, :block, across] = b.astype(BF16)
            hold_ref[y, block:, across] = part[proj_at:second].astype(BF16)
    y = lax.axis_index("yhi")
    keep_ref[...] = hold_ref[y]
    send_ref[...] = hold_ref[1 - y]


def base_rows(weight_ref, win_ref, out_ref):
    tok = win_ref.shape[0]
    spread = jnp.concatenate([win_ref[...]] * (LANE // tok), axis=0)
    out_ref[...] = lax.dot_general(weight_ref[...], spread, NT, preferred_element_type=F32)


def perturb(scale, base_ref, keep_ref, got_ref, out_ref, hold_ref):
    tall = keep_ref.shape[0]
    own_y = lax.axis_index("yhi")
    hold_ref[own_y] = keep_ref[...]
    hold_ref[1 - own_y] = got_ref[...]
    own = base_ref.shape[0]
    step = up8(own)
    tok = (tall - step) // PARTS
    rank = 4
    x = jnp.concatenate([hold_ref[0], hold_ref[1]], axis=1)
    wide = x.shape[1]
    source = lax.broadcasted_iota(jnp.int32, (wide, wide), 0)
    target = lax.broadcasted_iota(jnp.int32, (wide, wide), 1)
    place = ((source & 127) >> 3) * 32 + (source >> 7) * 8 + (source & 7)
    move = jnp.where(place == target, 1.0, 0.0).astype(BF16)
    x = jnp.dot(x, move, preferred_element_type=F32)
    cands = LANE // rank
    n = lax.broadcasted_iota(jnp.int32, (cands * tok, PARTS * LANE), 0)
    k = lax.broadcasted_iota(jnp.int32, (cands * tok, PARTS * LANE), 1)
    same = (n // tok) == ((k & 127) >> 2)
    base = jnp.concatenate([base_ref[...]] * (cands * tok // LANE), axis=1)
    for part in range(wide // LANE):
        tile = x[:, part * LANE : (part + 1) * LANE]
        b = tile[:step].astype(BF16)
        left = jnp.concatenate([b] * PARTS, axis=1)
        proj = jnp.concatenate(
            [tile[step + i * tok : step + (i + 1) * tok] for i in range(PARTS)], axis=1
        )
        right = jnp.where(same, jnp.concatenate([proj] * cands, axis=0), 0.0).astype(BF16)
        low = lax.dot_general(left, right, NT, preferred_element_type=F32)
        out = base + scale * low[:own]
        out_ref[:, part * cands * tok : (part + 1) * cands * tok] = out.astype(BF16)


OFFSETS = ((0, 5, -5), (1, 6, -4), (-1, 4, -6), (2, 7, -3), (-2, 3, -7), (8,))


def place_rows(chunks, rows_ref):
    groups, nz, _, _ = rows_ref.shape
    z = lax.axis_index("z")
    for ref, offsets in zip(chunks, OFFSETS):
        for i, offset in enumerate(offsets):
            place = lax.rem(z + (1 - 2 * lax.axis_index("core")) * offset + nz, nz)
            for g in range(groups):
                rows_ref[g, place] = ref[i, g]


def update_first(w_ref, *refs):
    chunks, out_ref, rows_ref = refs[:6], refs[6], refs[7]
    groups, nz, rows, width = rows_ref.shape
    place_rows(chunks, rows_ref)
    y, core = lax.axis_index("yhi"), lax.axis_index("core")
    tall = out_ref.shape[0]
    start = pl.multiple_of((1 - y) * tall, 8)
    left = jnp.concatenate(
        [w_ref[2 * g + 1 - core, pl.ds(start, tall), :] for g in range(groups)], axis=1
    )
    right = rows_ref[...].reshape(groups * nz * rows, width)
    out_ref[...] = jnp.dot(left, right, preferred_element_type=F32)


def update_rest(w_ref, *refs):
    chunks, out_refs, rows_ref = refs[:6], refs[6:9], refs[9]
    groups, nz, rows, width = rows_ref.shape
    place_rows(chunks, rows_ref)
    y, core = lax.axis_index("yhi"), lax.axis_index("core")
    tall = out_refs[0].shape[0]
    right = rows_ref[...].reshape(groups * nz * rows, width)
    for ref, yy, cc in zip(out_refs, (1 - y, y, y), (core, core, 1 - core)):
        start = pl.multiple_of(yy * tall, 8)
        left = jnp.concatenate(
            [w_ref[2 * g + cc, pl.ds(start, tall), :] for g in range(groups)], axis=1
        )
        ref[...] = jnp.dot(left, right, preferred_element_type=F32)


def shifted(value, offset):
    n = lax.axis_size("z")
    pairs = []
    for z in range(n):
        pairs.append((2 * z, 2 * ((z - offset) % n)))
        pairs.append((2 * z + 1, 2 * ((z + offset) % n) + 1))
    return lax.ppermute(value, ("z", "core"), pairs)


def swapped(value, axis):
    return lax.ppermute(value, axis, [(0, 1), (1, 0)])


def exchanged(value, axis):
    return lax.all_to_all(value, axis, 0, 0, tiled=True)


def step(window, weight, factor_a, factor_b, fitness):
    tok, depth = window.shape
    own = weight.shape[0]
    cands, rank, hidden = factor_b.shape
    groups, nz = lax.axis_size("grp"), lax.axis_size("z")
    nq = 4
    total = cands * groups * nz * nq
    rows = cands * rank
    width = depth // groups
    block = up8(own)
    tall = block + PARTS * tok
    shape = jax.ShapeDtypeStruct

    cut = call(
        cut_a,
        shape((groups, rows, width), BF16),
        (factor_a,),
        1 << 20,
        scratch=[pltpu.VMEM(factor_a.shape, BF16), pltpu.SemaphoreType.DMA],
        far=(0,),
    )
    mine = exchanged(cut, "grp")

    packed = call(
        pack_b,
        shape((nz * 2, rows, layout(own, tok)[-1]), BF16),
        (fitness, window, factor_a, factor_b),
        1 << 24,
        scratch=[
            pltpu.VMEM((rows, upl(hidden) + 2 * LANE), F32),
            pltpu.VMEM(window.shape, BF16),
            pltpu.VMEM(factor_a.shape, BF16),
            pltpu.VMEM(factor_b.shape, BF16),
            pltpu.SemaphoreType.DMA((3,)),
        ],
        smem=(0,),
        far=(1, 2, 3),
    )
    columns = exchanged(packed, ("z", "core"))
    weighted, keep, send = call(
        functools.partial(turn_b, own, tok),
        [
            shape((groups * 2, 2 * block, nz * rows), BF16),
            shape((tall, 2 * nz * rows), BF16),
            shape((tall, 2 * nz * rows), BF16),
        ],
        (columns,),
        1 << 24,
        scratch=[pltpu.VMEM((2, tall, 2 * nz * rows), BF16)],
    )
    weighted = exchanged(weighted, ("grp", "core"))
    got = swapped(send, "yhi")
    base = call(base_rows, shape((own, LANE), F32), (weight, window), 1 << 28)
    perturbed = call(
        functools.partial(perturb, 0.25 / math.sqrt(depth)),
        shape((own, cands * nz * nq * tok), BF16),
        (base, keep, got),
        1 << 30,
        scratch=[pltpu.VMEM((2, tall, 2 * nz * rows), BF16)],
    )

    mine = mine[None]
    far = shifted(mine, 5)
    near = jnp.concatenate([mine, far, shifted(mine, -5)], axis=0)
    up, down = shifted(near, 1), shifted(near, -1)
    up2, down2 = shifted(up, 1), shifted(down, -1)
    across = shifted(far, 3)
    part = shape((block, width), F32)
    operands = (weighted, near, up, down, up2, down2, across)
    held = [pltpu.VMEM((groups, nz, rows, width), BF16)]
    xx = call(update_first, part, operands, 1 << 28, scratch=held)
    xo, oo, ox = call(update_rest, [part] * 3, operands, 1 << 29, scratch=held)
    there = xo + swapped(xx, "core")
    here = oo + swapped(ox, "core")
    update = (here + swapped(there, "yhi"))[:own] * (0.5 / math.sqrt(total))
    return perturbed, update


def solution(mesh):
    split = Mesh(
        mesh.devices.reshape(mesh.shape["grp"], mesh.shape["shard"] // 4, 2, 2), GRP_SHARD
    )
    return jax.shard_map(
        step,
        mesh=split,
        in_specs=(
            P("grp", None),
            P(SHARD, None),
            P(GRP_SHARD, None, None),
            P(GRP_SHARD, None, None),
            P(GRP_SHARD),
        ),
        out_specs=(P(SHARD, "grp"), P(SHARD, "grp")),
        check_vma=False,
    )
```
